32 devices in a mesh: dp: 4 (over x, core), fsdp: 8 (over z, y).
Axes of the slice: x: 2, y: 2, z: 4, core: 2. Of those that a mesh axis runs over, the one named last changes fastest.
Arguments:
- hidden: bfloat16 [32, 256, 4096], P(('dp', 'fsdp')), may hold values from -40 to 40
- lengths: int32 [32], P(('dp', 'fsdp')), may hold values from 64 to 256
- list_ids: int32 [32], P('dp'), may hold values from 0 to 255, as said below
- list_owner: int32 [256], replicated, may hold values from 0 to 3, as said below
- attn_gain: float32 [4096], replicated, may hold values from 0.25 to 1.75
- final_gain: float32 [4096], replicated, may hold values from 0.25 to 1.75
- w_query: bfloat16 [4096, 2048], P('fsdp'), may hold values from -24 to 24
- w_key: bfloat16 [4096, 512], P('fsdp'), may hold values from -1 to 1
- w_value: bfloat16 [4096, 512], P('fsdp'), may hold values from -0.09375 to 0.09375
- w_out: bfloat16 [2048, 4096], P('fsdp'), may hold values from -0.125 to 0.125
Outputs:
- inbox: bfloat16 [4, 4, 4, 4096], P('dp', None, None, 'fsdp')
The draws below stay inside these ranges and needn't reach their ends.
Inputs may be any that keep to these rules, and one draw needn't show every extreme that they name: Positions from lengths[p] on are padding. `list_ids`: in each aligned block of 8 passages (those of one index of dp), at most 4 passages name lists of one owner, and in every block some owner is named by exactly 4 passages. `list_owner`: every owner holds exactly 64 lists.
All inputs are finite; a program needn't handle non-finite values.
Results may differ from the reference program's by a relative error of at most 0.0029.
The reference program's roundings to bfloat16 on the way (of `normed`, `key_rows`, `queries`, `weights`, `context` and `embedded`) count: a program that leaves them out, or rounds other values in their place, can miss the bound.
Values may be sent and summed in bfloat16 or wider, within the bound.
A program may use at most 64 MiB of HBM per device.

```python
import math
import jax
import jax.numpy as jnp
from jax import lax

D = 4096
HEADS = 16
KV_HEADS = 4
HEAD = 128
LEN = 256
PASSAGES = 32
LISTS = 256
CAP = 4
N_DP = 4


def owner_order(key):
    return jax.random.permutation(jax.random.fold_in(key, 7), LISTS)


def draw_list_owner(key, part):
    return (owner_order(key) % N_DP).astype(jnp.int32)


def draw_list_ids(key, part):
    inverse = jnp.argsort(owner_order(key))
    block_size = PASSAGES // N_DP
    slot_count = N_DP * CAP
    slot_owner = jnp.arange(slot_count) // CAP
    crowded = jax.random.randint(jax.random.fold_in(key, 8), (), 0, N_DP)

    def one_block(index):
        block_key = jax.random.fold_in(jax.random.fold_in(key, 9), index)
        noise = jax.random.randint(jax.random.fold_in(block_key, 1), (slot_count,), 0, 1 << 20)
        ranking = jnp.where(slot_owner == crowded, jnp.arange(slot_count), (noise + 1) * slot_count + jnp.arange(slot_count))
        chosen = slot_owner[jnp.argsort(ranking)[:block_size]]
        mixing = jax.random.randint(jax.random.fold_in(block_key, 2), (block_size,), 0, 1 << 20) * block_size + jnp.arange(block_size)
        owners = chosen[jnp.argsort(mixing)]
        choice_in_owner = jax.random.randint(jax.random.fold_in(block_key, 3), (block_size,), 0, LISTS // N_DP)
        return inverse[owners + N_DP * choice_in_owner]
    return jax.vmap(one_block)(jnp.arange(N_DP)).reshape(PASSAGES).astype(jnp.int32)


def key_base(key):
    drawn = jax.random.normal(jax.random.fold_in(key, 21), (D, KV_HEADS * HEAD), jnp.float32)
    return jnp.clip(drawn, -6.0, 6.0) / math.sqrt(D)


def draw_w_key(key, part):
    return key_base(key).astype(jnp.bfloat16)


def draw_w_query(key, part):
    drawn = jax.random.normal(jax.random.fold_in(key, 22), (D, HEADS * HEAD), jnp.float32)
    own_part = jnp.clip(drawn, -6.0, 6.0) / math.sqrt(D)
    return own_part.astype(jnp.bfloat16)


def draw_hidden(key, part):
    drawn = jax.random.normal(jax.random.fold_in(key, 31), (PASSAGES, LEN, D), jnp.float32)
    return jnp.clip(drawn, -6.0, 6.0).astype(jnp.bfloat16)


def set_ends(values, rng, low, largest):
    extent = values.shape
    index_at = [jax.random.randint(jax.random.fold_in(rng, axis), (), 0, extent[axis]) for axis in range(len(extent))]
    values = values.at[tuple(index_at)].set(low)
    longest = extent.index(max(extent))
    index_at[longest] = (index_at[longest] + 1) % extent[longest]
    return values.at[tuple(index_at)].set(largest)


def levels(own_key, extent, cuts, low, largest):
    factor_of, own = 1.0, jax.random.fold_in(own_key, 6)
    for dim, blocks in cuts:
        steps = jnp.exp(jax.random.uniform(jax.random.fold_in(own, dim), (blocks,), jnp.float32, low / len(cuts), largest / len(cuts)))
        factor_of = factor_of * jnp.repeat(steps, extent[dim] // blocks).reshape([-1 if axis == dim else 1 for axis in range(len(extent))])
    return factor_of


def centred(key, extent, scale, limit, split=(), kind=jnp.bfloat16):
    result = jax.random.normal(key, extent, jnp.float32) * scale
    if len(split) > 0:
        result = levels(key, extent, split, -0.22, 0.18) * result
    return jnp.clip(result, min=-limit, max=limit).astype(kind)


def setup_inputs(seed: int = 0) -> dict:
    seeds = jax.random.split(jax.random.key(seed), 11)
    return {
        "hidden": draw_hidden(jax.random.fold_in(seeds[10], 71), 0),
        "lengths": set_ends(jax.random.randint(seeds[1], (PASSAGES,), LEN // 4, LEN + 1), jax.random.fold_in(seeds[1], 1), LEN // 4, LEN).astype(jnp.int32),
        "list_ids": draw_list_ids(jax.random.fold_in(seeds[10], 71), 0),
        "list_owner": draw_list_owner(jax.random.fold_in(seeds[10], 71), 0),
        "attn_gain": jnp.clip(1.0 + 0.15 * jax.random.normal(seeds[4], (D,), jnp.float32), 0.25, 1.75),
        "final_gain": jnp.clip(1.0 + 0.15 * jax.random.normal(seeds[5], (D,), jnp.float32), 0.25, 1.75),
        "w_query": draw_w_query(jax.random.fold_in(seeds[10], 71), 0),
        "w_key": draw_w_key(jax.random.fold_in(seeds[10], 71), 0),
        "w_value": centred(seeds[8], (D, KV_HEADS * HEAD), D ** -0.5, 0.09375, ((0, 8),)),
        "w_out": centred(seeds[9], (HEADS * HEAD, D), (HEADS * HEAD) ** -0.5, 0.125, ((0, 8),)),
    }


def rope_tables(positions, head_width):
    halfway = head_width // 2
    frequency = 10000.0 ** (-jnp.arange(halfway, dtype=jnp.float32) * 2.0 / head_width)
    angles = positions.astype(jnp.float32)[..., None] * frequency
    return (jnp.cos(angles), jnp.sin(angles))

def rotate(vectors, cosine_table, sine_table):
    halfway = vectors.shape[-1] // 2
    first_half = vectors[..., :halfway]
    second_half = vectors[..., halfway:]
    return jnp.concatenate([first_half * cosine_table - second_half * sine_table, second_half * cosine_table + first_half * sine_table], axis=-1)

def reference(hidden, lengths, list_ids, list_owner, attn_gain, final_gain, w_query, w_key, w_value, w_out):
    cosine_table, sine_table = rope_tables(jnp.arange(LEN), HEAD)

    def embed_one(inputs):
        passage, length = inputs
        floats = passage.astype(jnp.float32)
        normed = (floats * lax.rsqrt(lax.optimization_barrier(jnp.mean(floats * floats, axis=-1, keepdims=True)) + 1e-05) * attn_gain).astype(jnp.bfloat16)
        key_sum = jnp.dot(normed, w_key, preferred_element_type=jnp.float32).reshape(LEN, KV_HEADS, HEAD)
        key_rows = rotate(key_sum, cosine_table[:, None, :], sine_table[:, None, :]).astype(jnp.bfloat16)
        value_rows = jnp.dot(normed, w_value, preferred_element_type=jnp.float32).reshape(LEN, KV_HEADS, HEAD)
        last_position = length - 1
        last_normed = lax.dynamic_index_in_dim(normed, last_position, 0, keepdims=False)
        last_input = lax.dynamic_index_in_dim(passage, last_position, 0, keepdims=False).astype(jnp.float32)
        query_sum = jnp.dot(last_normed, w_query, preferred_element_type=jnp.float32).reshape(HEADS, HEAD)
        query_cos, query_sin = rope_tables(last_position[None], HEAD)
        queries = (rotate(query_sum, query_cos, query_sin) * (1.0 / math.sqrt(HEAD))).astype(jnp.bfloat16)
        grouped = queries.reshape(KV_HEADS, HEADS // KV_HEADS, HEAD).astype(jnp.float32)
        scores = jnp.einsum('kgd,tkd->kgt', grouped, key_rows.astype(jnp.float32))
        visible = jnp.arange(LEN)[None, None, :] < length
        scores = jnp.where(visible, scores, -jnp.inf)
        powers = jnp.exp(scores - lax.optimization_barrier(jnp.max(scores, axis=-1, keepdims=True)))
        weights = (powers / lax.optimization_barrier(jnp.sum(powers, axis=-1, keepdims=True))).astype(jnp.bfloat16)
        context = jnp.einsum('kgt,tkd->kgd', weights.astype(jnp.float32), value_rows, precision=lax.Precision.HIGHEST)
        context = context.reshape(HEADS * HEAD).astype(jnp.bfloat16)
        residual = last_input + jnp.dot(context, w_out, preferred_element_type=jnp.float32)
        scaled = residual * final_gain
        return (scaled * lax.rsqrt(jnp.mean(scaled * scaled) + 1e-06)).astype(jnp.bfloat16)
    embedded = lax.map(embed_one, (hidden, lengths))
    block_size = PASSAGES // N_DP
    owners = list_owner[list_ids].reshape(N_DP, block_size)
    owner_marks = (owners[:, :, None] == jnp.arange(N_DP)[None, None, :]).astype(jnp.int32)
    slot_rank = lax.optimization_barrier(jnp.sum((jnp.cumsum(owner_marks, axis=1) - owner_marks) * owner_marks, axis=2))
    select = ((owners[:, None, None, :] == jnp.arange(N_DP)[None, :, None, None]) & (slot_rank[:, None, None, :] == jnp.arange(CAP)[None, None, :, None])).astype(jnp.float32)
    grouped_rows = embedded.reshape(N_DP, block_size, D).astype(jnp.float32)
    inbox = jnp.einsum('josr,jrd->ojsd', select, grouped_rows, precision=lax.Precision.HIGHEST)
    return inbox.astype(jnp.bfloat16)
```

```python
import functools
import math

import jax
import jax.numpy as jnp
import numpy as np
from jax import lax
from jax.experimental import pallas as pl
from jax.experimental.pallas import tpu as pltpu
from jax.sharding import PartitionSpec as P

HEADS = 16
KV_HEADS = 4
HEAD = 128
GROUP = HEADS // KV_HEADS
CORES = 2
MY_HEADS = HEADS // CORES
MY_KV = KV_HEADS // CORES
UNITS = 8
MESH = pl.DeviceIdType.MESH
F32 = jnp.float32
BF16 = jnp.bfloat16


def rope_tables(seq_len):
    half = HEAD // 2
    exponent = -np.arange(half, dtype=np.float32) * np.float32(2.0) / np.float32(HEAD)
    frequency = (np.float64(10000.0) ** exponent.astype(np.float64)).astype(np.float32)
    angles = (np.arange(seq_len, dtype=np.float32)[:, None] * frequency).astype(np.float64)
    cosine, sine = np.cos(angles), np.sin(angles)
    return (
        np.concatenate([cosine, cosine], axis=1).astype(np.float32),
        np.concatenate([-sine, sine], axis=1).astype(np.float32),
    )


def key_chunks(n):
    if n <= 8:
        return ((0, 1), (1, 2), (2, 3)), ((0, 1), (1, 2))
    return ((0, 3),), ((0, 2),)


def kernel(
    n_dp, n,
    lengths_hbm, ids_hbm,
    owners_hbm, hidden_hbm, again_hbm, fgain_hbm, cos_hbm, sin_hbm, wq_hbm, wk_hbm, wv_hbm, wo_hbm,
    out_ref,
    lengths, list_ids,
    hid, normed, squares, again, fgain, cos_t, sin_t, wq, wk, wv, wo,
    owners, acc, last_in,
    x_send, x_recv, q_send, q_recv, u_send, u_recv, mixed, c_send, c_recv, o_send, o_recv,
    e_send, e_recv, s_send, s_recv,
    load_sem, a2a_send, a2a_recv, norm_send, norm_recv,
    z_s, y_s, x_s, z_r, y_r, x_r,
):
    dp = lax.axis_index("dp")
    f = lax.axis_index("fsdp")
    seq_len, width = hid.shape
    slab = width // n
    depth = n // 2
    total = n_dp * n
    half = n // 2
    cap = out_ref.shape[2]
    a, b = f // 2, f % 2
    core, x_bit = dp % 2, (dp // 2) % 2
    base = dp - core
    partner = base + 1 - core
    x_peer = dp + 2 - 4 * x_bit
    me = dp * n + f
    key_width = wk.shape[2]
    query_width = wq.shape[1]

    def lanes(index, size):
        return pl.ds(pl.multiple_of(index * size, size), size)

    sources = (
        wk_hbm.at[:, lanes(core, key_width)], lengths_hbm, hidden_hbm.at[0], again_hbm,
        wq_hbm.at[:, lanes(core, query_width)], cos_hbm, sin_hbm, wv_hbm.at[:, lanes(core, key_width)], wo_hbm,
        fgain_hbm.at[:, lanes(f, slab)], owners_hbm, ids_hbm,
    )
    targets = (wk.at[f], lengths, hid, again, wq, cos_t, sin_t, wv, wo, fgain, owners, list_ids)
    loads = [
        pltpu.make_async_copy(s, t, load_sem.at[i])
        for i, (s, t) in enumerate(zip(sources, targets))
    ]

    def wrap(index, size):
        return jnp.where(index >= size, index - size, index)

    def each(low, high, body):
        if high <= 8:
            for t in range(low, high):
                body(t)
        else:
            lax.fori_loop(low, high, lambda t, c: (body(t), c)[1], 0)

    def everyone(body):
        for t in range(n_dp):
            o = wrap(dp + t, n_dp)
            each(1 if t == 0 else 0, n, lambda i: body(o, wrap(f + i, n)))

    barrier = pltpu.get_barrier_semaphore()
    everyone(lambda o, g: pl.semaphore_signal(barrier, inc=1, device_id=(o, g), device_id_type=MESH))
    for load in loads:
        load.start()

    unit = slab // UNITS
    alone, shared = key_chunks(n)
    chunks = [(2, 3, lo, hi) for lo, hi in alone] + [(0, 0, lo, hi) for lo, hi in shared]
    n_alone = len(alone)

    def piece(pa, pb, c, column, send_sem, recv_sem, device):
        first, step, lo, hi = chunks[c]
        start = (first + step * column + lo) * unit
        part = wk.at[pa * 2 + pb, pl.ds(pl.multiple_of(start, unit), (hi - lo) * unit), :]
        return pltpu.make_async_remote_copy(
            src_ref=part, dst_ref=part, send_sem=send_sem, recv_sem=recv_sem,
            device_id=device, device_id_type=MESH,
        )

    def far(t):
        return wrap(a + t, depth)

    def along_z(t, c):
        return piece(a, b, c, x_bit, z_s.at[t, c], z_r.at[a, c], (dp, far(t) * 2 + b))

    def from_z(pa, c):
        return piece(pa, b, c, x_bit, z_s.at[0, c], z_r.at[pa, c], (dp, f))

    def along_y(pa, c):
        return piece(pa, b, c, x_bit, y_s.at[pa, c], y_r.at[pa, c], (dp, 2 * a + 1 - b))

    def from_y(pa, c):
        return piece(pa, 1 - b, c, x_bit, y_s.at[pa, c], y_r.at[pa, c], (dp, f))

    def along_x(pa, pb, c):
        return piece(pa, pb, c, x_bit, x_s.at[pa * 2 + pb, c], x_r.at[pa * 2 + pb, c], (x_peer, f))

    def from_x(pa, pb, c):
        return piece(pa, pb, c, 1 - x_bit, x_s.at[pa * 2 + pb, c], x_r.at[pa * 2 + pb, c], (dp, f))

    def others(body):
        each(1, depth, lambda t: body(far(t)))

    def give(slot, src, dst, device):
        pltpu.make_async_remote_copy(
            src_ref=src, dst_ref=dst, send_sem=a2a_send.at[slot],
            recv_sem=a2a_recv.at[slot], device_id=device, device_id_type=MESH,
        ).start()

    def exchange(slot, send, recv):
        each(1, n, lambda t: give(slot, send.at[wrap(f + t, n)], recv.at[f], (dp, wrap(f + t, n))))
        recv[f] = send[f]

    def arrived(slot, recv, count):
        blocks = recv.at[pl.ds(0, count)]
        pltpu.make_async_copy(blocks, blocks, a2a_recv.at[slot]).wait()

    def sent(slot, recv, count):
        blocks = recv.at[pl.ds(0, count)]
        pltpu.make_async_copy(blocks, blocks, a2a_send.at[slot]).wait()

    with jax.named_scope("p_barrier"):
        pl.semaphore_wait(barrier, total - 1)
    with jax.named_scope("p_wkload"):
        loads[0].wait()
    for c in range(len(chunks)):
        along_y(a, c).start()
        each(1, depth, lambda t: along_z(t, c).start())

    with jax.named_scope("p_hidload"):
        for load in loads[1:4]:
            load.wait()
    length = lengths[0]
    picks = lax.broadcasted_iota(jnp.int32, (16, seq_len), 1) == length - 1
    picks = jnp.where(picks, 1.0, 0.0).astype(BF16)
    row = jnp.concatenate(
        [
            jnp.dot(picks, hid[:, g * slab:(g + 1) * slab], preferred_element_type=F32)[:1]
            for g in range(n)
        ],
        axis=1,
    )
    scale = lax.rsqrt(jnp.mean(row * row, axis=-1, keepdims=True) + 1e-05)
    row_normed = (row * scale * again[...]).astype(BF16).astype(F32)
    size = jnp.full((1, 128), length, jnp.int32).astype(F32)
    for g in range(n):
        x_send[g, :, :slab] = row_normed[:, g * slab:(g + 1) * slab]
        x_send[g, :, slab:2 * slab] = row[:, g * slab:(g + 1) * slab]
        x_send[g, :, 2 * slab:] = size
    place = core * n + f
    with jax.named_scope("p_x"):
        each(1, n, lambda t: give(0, x_send.at[wrap(f + t, n)], x_recv.at[place], (dp, wrap(f + t, n))))
        each(0, n, lambda t: give(0, x_send.at[wrap(f + t, n)], x_recv.at[place], (partner, wrap(f + t, n))))
        x_recv[place] = x_send[f]

    block = 16
    blocks = seq_len // block

    def square(i, carry):
        window = pl.ds(pl.multiple_of(i * block, block), block)
        x = hid[window, :].astype(F32)
        x = x * x
        lane_sum = x[:, :128]
        for k in range(1, width // 128):
            lane_sum += x[:, k * 128:(k + 1) * 128]
        squares[window, :] = lane_sum
        return carry

    with jax.named_scope("p_norm"):
        lax.fori_loop(0, blocks, square, 0)
        means = jnp.sum(squares[...], axis=-1, keepdims=True) / width
        squares[...] = jnp.broadcast_to(lax.rsqrt(means + 1e-05), squares.shape)

        def normalise(i, carry):
            window = pl.ds(pl.multiple_of(i * block, block), block)
            into = pl.ds(pl.multiple_of(core * seq_len + i * block, block), block)
            r = squares[window, :1]
            normed[into, :] = (hid[window, :].astype(F32) * r * again[...]).astype(BF16)
            return carry

        quarter = seq_len // 4

        def hand(k):
            part = normed.at[pl.ds(pl.multiple_of(core * seq_len + k * quarter, quarter), quarter), :]
            return pltpu.make_async_remote_copy(
                src_ref=part, dst_ref=part, send_sem=norm_send.at[k], recv_sem=norm_recv.at[k],
                device_id=(partner, f), device_id_type=MESH,
            )

        for k in range(4):
            lax.fori_loop(k * blocks // 4, (k + 1) * blocks // 4, normalise, 0)
            hand(k).start()

    def handed():
        for k in range(4):
            part = normed.at[pl.ds(pl.multiple_of((1 - core) * seq_len + k * quarter, quarter), quarter), :]
            pltpu.make_async_copy(part, part, norm_recv.at[k]).wait()

    def partial_queries():
        loads[4].wait()
        arrived(0, x_recv, 2 * n - 1)
        x_all = jnp.concatenate([x_recv[k, :, :slab] for k in range(2 * n)], axis=0).astype(BF16)
        for h in range(MY_HEADS):
            part = jnp.dot(x_all, wq[:, h * HEAD:(h + 1) * HEAD], preferred_element_type=F32)
            for s in range(CORES):
                q_send[pl.ds(s * MY_HEADS + h, n, stride=CORES * MY_HEADS), :] = part[s * n:(s + 1) * n]
        rows = CORES * MY_HEADS

        def at(g):
            return pl.ds(pl.multiple_of(g * rows, rows), rows)

        each(1, n, lambda t: give(1, q_send.at[at(wrap(f + t, n))], q_recv.at[f], (dp, wrap(f + t, n))))
        q_recv[f] = q_send[at(f), :]

    def codes():
        for load in loads[5:]:
            load.wait()
        for i in range(n):
            last_in[i:i + 1, :] = x_recv[core * n + i][:, slab:2 * slab]
        lists = lax.broadcasted_iota(jnp.int32, (n, owners.shape[1]), 1)
        rows = lax.broadcasted_iota(jnp.int32, (n, owners.shape[1]), 0)
        ids = jnp.zeros((n, owners.shape[1]), jnp.int32)
        for r in range(n):
            ids = jnp.where(rows == r, list_ids[r], ids)
        owner = jnp.sum(jnp.where(lists == ids, owners[...], 0).astype(F32), axis=1, keepdims=True)
        lane = lax.broadcasted_iota(jnp.int32, (n, 128), 1)
        line = lax.broadcasted_iota(jnp.int32, (n, 128), 0)
        owner_row = jnp.sum(jnp.where(lane == line, owner, 0.0), axis=0, keepdims=True)
        earlier = jnp.where((owner_row == owner) & (lane < line), 1.0, 0.0)
        slot = jnp.sum(earlier, axis=1, keepdims=True)
        e_send[:, slab:] = jnp.broadcast_to(owner * cap + slot, (n, 128))

    split = 2 * unit
    parted = split % 128 == 0

    def accumulate(s, low, high):
        columns = pl.ds(pl.multiple_of(s * slab + low, 128), high - low)
        acc[...] += jnp.dot(normed[:, columns], wk[s, low:high, :], preferred_element_type=F32)

    def own_plane(c):
        from_y(a, c).wait_recv()
        if c < n_alone:
            along_x(a, 1 - b, c).start()

    def pass_z(c):
        def body(pa):
            from_z(pa, c).wait_recv()
            along_y(pa, c).start()
            if c < n_alone:
                along_x(pa, b, c).start()
        others(body)

    def pass_y(c):
        def body(pa):
            from_y(pa, c).wait_recv()
            if c < n_alone:
                along_x(pa, 1 - b, c).start()
        others(body)

    with jax.named_scope("g_0"):
        own_plane(0)
        pass_z(0)
    acc[...] = jnp.zeros_like(acc)
    for c in range(1, len(chunks)):
        with jax.named_scope(f"g_z{c}"):
            own_plane(c)
            pass_z(c)
        with jax.named_scope(f"g_y{c}"):
            pass_y(c - 1)
        if c == 1:
            with jax.named_scope("g_q"):
                partial_queries()
                codes()
                handed()
                accumulate(f, 0, slab)

    def first_part(pa, pb):
        for c in range(n_alone):
            from_x(pa, pb, c).wait_recv()
        if parted:
            accumulate(pa * 2 + pb, split, slab)

    with jax.named_scope("g_x"):
        first_part(a, 1 - b)
        others(lambda pa: (first_part(pa, b), first_part(pa, 1 - b)) and None)
    with jax.named_scope("g_last"):
        pass_y(len(chunks) - 1)
    low, high = (0, split) if parted else (0, slab)
    accumulate(a * 2 + 1 - b, low, high)
    others(lambda pa: (accumulate(pa * 2 + b, low, high), accumulate(pa * 2 + 1 - b, low, high)) and None)

    with jax.named_scope("p_qwait"):
        arrived(1, q_recv, n - 1)
    queries = jnp.sum(q_recv[...], axis=0)
    rows = CORES * MY_HEADS
    upper = lax.broadcasted_iota(jnp.int32, (rows, 1), 0) >= MY_HEADS
    size_of = [x_recv[s * n + f][:, 2 * slab:2 * slab + 1] for s in range(CORES)]
    turns = []
    for s in range(CORES):
        token = lax.broadcasted_iota(jnp.int32, cos_t.shape, 0).astype(F32)
        at_last = token == size_of[s] - 1.0
        turns.append([
            jnp.sum(jnp.where(at_last, table[...], 0.0), axis=0, keepdims=True) for table in (cos_t, sin_t)
        ])
    q_cos = jnp.where(upper, turns[1][0], turns[0][0])
    q_sin = jnp.where(upper, turns[1][1], turns[0][1])
    queries = queries * q_cos + pltpu.roll(queries, HEAD // 2, 1) * q_sin
    queries = (queries * (1.0 / math.sqrt(HEAD))).astype(BF16)

    scores = jnp.zeros((rows, seq_len), F32)
    key_of = lax.broadcasted_iota(jnp.int32, scores.shape, 0) // GROUP
    for s in range(CORES):
        for kv in range(MY_KV):
            keys = acc[s * seq_len:(s + 1) * seq_len, kv * HEAD:(kv + 1) * HEAD]
            keys = (keys * cos_t[...] + pltpu.roll(keys, HEAD // 2, 1) * sin_t[...]).astype(BF16)
            part = lax.dot_general(queries, keys, (((1,), (1,)), ((), ())), preferred_element_type=F32)
            scores = jnp.where(key_of == s * MY_KV + kv, part, scores)
    token = lax.broadcasted_iota(jnp.int32, scores.shape, 1).astype(F32)
    visible = token < jnp.where(upper, size_of[1], size_of[0])
    scores = jnp.where(visible, scores, -jnp.inf)
    powers = jnp.exp(scores - jnp.max(scores, axis=-1, keepdims=True))
    weights = powers / jnp.sum(powers, axis=-1, keepdims=True)
    weights = jnp.concatenate(
        [jnp.where(upper, 0.0, weights), jnp.where(upper, weights, 0.0)], axis=1
    ).astype(BF16)

    def weighted(g):
        return jnp.dot(weights, normed[:, lanes(g, slab)], preferred_element_type=F32)

    with jax.named_scope("p_u"):
        for t in range(1, n):
            g = wrap(f + t, n)
            u_send[g] = weighted(g)
            give(2, u_send.at[g], u_recv.at[f], (dp, g))
        u_recv[f] = weighted(f)
    with jax.named_scope("p_uwait"):
        arrived(2, u_recv, n - 1)
    sums = u_recv[...].reshape(n * rows, slab)
    top = sums.astype(BF16)
    rest = sums - top.astype(F32)
    middle = rest.astype(BF16)
    low_part = (rest - middle.astype(F32)).astype(BF16)
    values = wv[...]
    product = (
        jnp.dot(low_part, values, preferred_element_type=F32)
        + jnp.dot(middle, values, preferred_element_type=F32)
    ) + jnp.dot(top, values, preferred_element_type=F32)
    for kv in range(MY_KV):
        mixed[kv] = product[:, kv * HEAD:(kv + 1) * HEAD]

    share = HEADS * HEAD // n
    for s in range(CORES):
        for h in range(MY_HEADS):
            part = mixed[h // GROUP, pl.ds(s * MY_HEADS + h, n, stride=rows), :]
            if share >= HEAD:
                at = h * HEAD % share
                c_send[s * half + h * HEAD // share, :, at:at + HEAD] = part
            else:
                pieces = HEAD // share
                for i in range(pieces):
                    c_send[s * half + h * pieces + i] = part[:, i * share:(i + 1) * share]

    mine = f // half == core
    other_core = 1 - core

    def context_to(s, t):
        k = lax.rem(f + t, half)
        give(3, c_send.at[s * half + k], c_recv.at[f], (base + s, core * half + k))

    each(1, half, lambda t: context_to(core, t))
    each(0, half, lambda t: context_to(other_core, t))

    @pl.when(mine)
    def _():
        c_recv[f] = c_send[core * half + lax.rem(f, half)]
        arrived(3, c_recv, n - 1)

    @pl.when(jnp.logical_not(mine))
    def _():
        context_to(core, 0)
        arrived(3, c_recv, n)

    context = jnp.sum(c_recv[...], axis=0).astype(BF16)

    def projected(g):
        return jnp.dot(context, wo[:, lanes(g, slab)], preferred_element_type=F32)

    with jax.named_scope("p_o"):
        for t in range(1, n):
            g = wrap(f + t, n)
            o_send[g] = projected(g)
            give(4, o_send.at[g], o_recv.at[f], (dp, g))
        o_recv[f] = projected(f)
    with jax.named_scope("p_owait"):
        arrived(4, o_recv, n - 1)
    scaled = (last_in[...] + jnp.sum(o_recv[...], axis=0)) * fgain[...]
    lane = lax.broadcasted_iota(jnp.int32, (n, 128), 1)
    line = lax.broadcasted_iota(jnp.int32, (n, 128), 0)
    summed = jnp.sum(scaled * scaled, axis=1, keepdims=True)
    s_send[...] = jnp.sum(jnp.where(lane == line, summed, 0.0), axis=0, keepdims=True)
    everyone(lambda o, g: give(6, s_send, s_recv.at[me], (o, g)))
    e_send[:, :slab] = scaled
    for t in range(1, n_dp):
        give(5, e_send, e_recv.at[dp], (wrap(dp + t, n_dp), f))
    s_recv[me] = s_send[...]
    e_recv[dp] = e_send[...]
    with jax.named_scope("p_ewait"):
        arrived(5, e_recv, n_dp - 1)
        arrived(6, s_recv, total - 1)

    first = (dp * cap).astype(F32)
    for j in range(n_dp):
        sum_row = jnp.sum(s_recv[j * n:(j + 1) * n], axis=0)
        squared = jnp.sum(jnp.where(lane == line, sum_row, 0.0), axis=1, keepdims=True)
        embedded = e_recv[j, :, :slab] * lax.rsqrt(squared / width + 1e-06)
        embedded = embedded.astype(BF16).astype(F32)
        owner_slot = e_recv[j, :, slab:slab + 1]
        for s in range(cap):
            kept = jnp.where(owner_slot == first + s, embedded, 0.0)
            out_ref[0, j, s:s + 1, :] = jnp.sum(kept, axis=0, keepdims=True).astype(BF16)

    with jax.named_scope("p_sent"):
        sent(0, x_recv, 2 * n - 1)
        for slot, recv in ((1, q_recv), (2, u_recv), (4, o_recv)):
            sent(slot, recv, n - 1)

        @pl.when(mine)
        def _():
            sent(3, c_recv, n - 1)

        @pl.when(jnp.logical_not(mine))
        def _():
            sent(3, c_recv, n)

        sent(5, e_recv, n_dp - 1)
        sent(6, s_recv, total - 1)
        for k in range(4):
            hand(k).wait_send()
    with jax.named_scope("p_drain"):
        for c in range(len(chunks)):
            each(1, depth, lambda t: along_z(t, c).wait_send())
            each(0, depth, lambda t: along_y(far(t), c).wait_send())
            if c < n_alone:
                along_x(a, 1 - b, c).wait_send()
                others(lambda pa: (along_x(pa, b, c).wait_send(), along_x(pa, 1 - b, c).wait_send()) and None)


def local(
    n_dp, n,
    hidden, lengths, list_ids, list_owner, attn_gain, final_gain, w_query, w_key, w_value, w_out,
):
    _, seq_len, width = hidden.shape
    slab = width // n
    depth = n // 2
    cap = max(2, 2 * n // n_dp)
    share = HEADS * HEAD // n
    cosine, sine = rope_tables(seq_len)
    alone, shared = key_chunks(n)
    dma = pltpu.SemaphoreType.DMA
    any_spec = pl.BlockSpec(memory_space=pl.ANY)
    vmem = pltpu.VMEM
    key_width = w_key.shape[1] // CORES
    rows = CORES * MY_HEADS
    return pl.pallas_call(
        functools.partial(kernel, n_dp, n),
        out_shape=jax.ShapeDtypeStruct((1, n_dp, cap, slab), BF16),
        in_specs=[any_spec] * 12,
        out_specs=pl.BlockSpec(memory_space=pltpu.VMEM),
        scratch_shapes=[
            pltpu.SMEM(lengths.shape, jnp.int32),
            pltpu.SMEM(list_ids.shape, jnp.int32),
            vmem((seq_len, width), BF16),
            vmem((CORES * seq_len, width), BF16),
            vmem((seq_len, 128), F32),
            vmem((1, width), F32),
            vmem((1, slab), F32),
            vmem((seq_len, HEAD), F32),
            vmem((seq_len, HEAD), F32),
            vmem((w_query.shape[0], w_query.shape[1] // CORES), BF16),
            vmem((n, slab, key_width), BF16),
            vmem((slab, key_width), BF16),
            vmem(w_out.shape, BF16),
            vmem((1, list_owner.shape[0]), jnp.int32),
            vmem((CORES * seq_len, key_width), F32),
            vmem((n, slab), F32),
            vmem((n, 1, 2 * slab + 128), F32),
            vmem((CORES * n, 1, 2 * slab + 128), F32),
            vmem((n * rows, HEAD), F32),
            vmem((n, rows, HEAD), F32),
            vmem((n, rows, slab), F32),
            vmem((n, rows, slab), F32),
            vmem((MY_KV, n * rows, HEAD), F32),
            vmem((n, n, share), F32),
            vmem((n, n, share), F32),
            vmem((n, n, slab), F32),
            vmem((n, n, slab), F32),
            vmem((n, slab + 128), F32),
            vmem((n_dp, n, slab + 128), F32),
            vmem((1, 128), F32),
            vmem((n_dp * n, 1, 128), F32),
            dma((12,)),
            dma((7,)),
            dma((7,)),
            dma((4,)),
            dma((4,)),
            dma((depth, len(alone) + len(shared))),
            dma((depth, len(alone) + len(shared))),
            dma((n, len(alone))),
            dma((depth, len(alone) + len(shared))),
            dma((depth, len(alone) + len(shared))),
            dma((n, len(alone))),
        ],
        compiler_params=pltpu.CompilerParams(
            collective_id=0, has_side_effects=True, vmem_limit_bytes=67043328
        ),
    )(
        lengths, list_ids,
        list_owner.reshape(1, -1), hidden, attn_gain.reshape(1, width), final_gain.reshape(1, width),
        cosine, sine, w_query, w_key, w_value, w_out,
    )


def solution(mesh):
    in_specs = (
        P(("dp", "fsdp"), None, None),
        P(("dp", "fsdp")),
        P("dp"),
        P(),
        P(),
        P(),
        P("fsdp", None),
        P("fsdp", None),
        P("fsdp", None),
        P("fsdp", None),
    )
    out_specs = P("dp", None, None, "fsdp")
    body = functools.partial(local, mesh.shape["dp"], mesh.shape["fsdp"])
    return jax.shard_map(body, mesh=mesh, in_specs=in_specs, out_specs=out_specs, check_vma=False)
```

```python
import functools
import math

import jax
import jax.numpy as jnp
import numpy as np
from jax import lax
from jax.experimental import pallas as pl
from jax.experimental.pallas import tpu as pltpu
from jax.sharding import PartitionSpec as P

HEADS = 16
KV_HEADS = 4
HEAD = 128
GROUP = HEADS // KV_HEADS
CORES = 2
MY_HEADS = HEADS // CORES
MY_KV = KV_HEADS // CORES
UNITS = 8
MESH = pl.DeviceIdType.MESH
F32 = jnp.float32
BF16 = jnp.bfloat16


def rope_tables(seq_len):
    half = HEAD // 2
    exponent = -np.arange(half, dtype=np.float32) * np.float32(2.0) / np.float32(HEAD)
    frequency = (np.float64(10000.0) ** exponent.astype(np.float64)).astype(np.float32)
    angles = (np.arange(seq_len, dtype=np.float32)[:, None] * frequency).astype(np.float64)
    cosine, sine = np.cos(angles), np.sin(angles)
    return (
        np.concatenate([cosine, cosine], axis=1).astype(np.float32),
        np.concatenate([-sine, sine], axis=1).astype(np.float32),
    )


def key_chunks(n):
    if n <= 8:
        return ((0, 1), (1, 2), (2, 3)), ((0, 1), (1, 2))
    return ((0, 3),), ((0, 2),)


def kernel(
    n_dp, n,
    lengths_hbm, ids_hbm,
    owners_hbm, hidden_hbm, again_hbm, fgain_hbm, cos_hbm, sin_hbm, wq_hbm, wk_hbm, wv_hbm, wo_hbm,
    out_ref,
    lengths, list_ids,
    hid, normed, squares, again, fgain, cos_t, sin_t, wq, wk, wv, wo,
    owners, acc, last_in,
    x_send, x_recv, q_send, q_recv, u_send, u_recv, mixed, c_send, c_recv, o_send, o_recv,
    e_send, e_recv, s_send, s_recv,
    load_sem, a2a_send, a2a_recv, norm_send, norm_recv,
    z_s, y_s, x_s, z_r, y_r, x_r,
):
    dp = lax.axis_index("dp")
    f = lax.axis_index("fsdp")
    seq_len, width = hid.shape
    slab = width // n
    depth = n // 2
    total = n_dp * n
    half = n // 2
    cap = out_ref.shape[2]
    a, b = f // 2, f % 2
    core, x_bit = dp % 2, (dp // 2) % 2
    base = dp - core
    partner = base + 1 - core
    x_peer = dp + 2 - 4 * x_bit
    me = dp * n + f
    key_width = wk.shape[2]
    query_width = wq.shape[1]

    def lanes(index, size):
        return pl.ds(pl.multiple_of(index * size, size), size)

    sources = (
        wk_hbm.at[:, lanes(core, key_width)], lengths_hbm, hidden_hbm.at[0], again_hbm,
        wq_hbm.at[:, lanes(core, query_width)], cos_hbm, sin_hbm, wv_hbm.at[:, lanes(core, key_width)], wo_hbm,
        fgain_hbm.at[:, lanes(f, slab)], owners_hbm, ids_hbm,
    )
    targets = (wk.at[f], lengths, hid, again, wq, cos_t, sin_t, wv, wo, fgain, owners, list_ids)
    loads = [
        pltpu.make_async_copy(s, t, load_sem.at[i])
        for i, (s, t) in enumerate(zip(sources, targets))
    ]

    def wrap(index, size):
        return jnp.where(index >= size, index - size, index)

    def each(low, high, body):
        if high <= 8:
            for t in range(low, high):
                body(t)
        else:
            lax.fori_loop(low, high, lambda t, c: (body(t), c)[1], 0)

    def everyone(body):
        for t in range(n_dp):
            o = wrap(dp + t, n_dp)
            each(1 if t == 0 else 0, n, lambda i: body(o, wrap(f + i, n)))

    barrier = pltpu.get_barrier_semaphore()
    everyone(lambda o, g: pl.semaphore_signal(barrier, inc=1, device_id=(o, g), device_id_type=MESH))
    for load in loads:
        load.start()

    unit = slab // UNITS
    alone, shared = key_chunks(n)
    chunks = [(2, 3, lo, hi) for lo, hi in alone] + [(0, 0, lo, hi) for lo, hi in shared]
    n_alone = len(alone)

    def piece(pa, pb, c, column, send_sem, recv_sem, device):
        first, step, lo, hi = chunks[c]
        start = (first + step * column + lo) * unit
        part = wk.at[pa * 2 + pb, pl.ds(pl.multiple_of(start, unit), (hi - lo) * unit), :]
        return pltpu.make_async_remote_copy(
            src_ref=part, dst_ref=part, send_sem=send_sem, recv_sem=recv_sem,
            device_id=device, device_id_type=MESH,
        )

    def far(t):
        return wrap(a + t, depth)

    def along_z(t, c):
        return piece(a, b, c, x_bit, z_s.at[t, c], z_r.at[a, c], (dp, far(t) * 2 + b))

    def from_z(pa, c):
        return piece(pa, b, c, x_bit, z_s.at[0, c], z_r.at[pa, c], (dp, f))

    def along_y(pa, c):
        return piece(pa, b, c, x_bit, y_s.at[pa, c], y_r.at[pa, c], (dp, 2 * a + 1 - b))

    def from_y(pa, c):
        return piece(pa, 1 - b, c, x_bit, y_s.at[pa, c], y_r.at[pa, c], (dp, f))

    def along_x(pa, pb, c):
        return piece(pa, pb, c, x_bit, x_s.at[pa * 2 + pb, c], x_r.at[pa * 2 + pb, c], (x_peer, f))

    def from_x(pa, pb, c):
        return piece(pa, pb, c, 1 - x_bit, x_s.at[pa * 2 + pb, c], x_r.at[pa * 2 + pb, c], (dp, f))

    def others(body):
        each(1, depth, lambda t: body(far(t)))

    def give(slot, src, dst, device):
        pltpu.make_async_remote_copy(
            src_ref=src, dst_ref=dst, send_sem=a2a_send.at[slot],
            recv_sem=a2a_recv.at[slot], device_id=device, device_id_type=MESH,
        ).start()

    def exchange(slot, send, recv):
        each(1, n, lambda t: give(slot, send.at[wrap(f + t, n)], recv.at[f], (dp, wrap(f + t, n))))
        recv[f] = send[f]

    def arrived(slot, recv, count):
        blocks = recv.at[pl.ds(0, count)]
        pltpu.make_async_copy(blocks, blocks, a2a_recv.at[slot]).wait()

    def sent(slot, recv, count):
        blocks = recv.at[pl.ds(0, count)]
        pltpu.make_async_copy(blocks, blocks, a2a_send.at[slot]).wait()

    with jax.named_scope("p_barrier"):
        pl.semaphore_wait(barrier, total - 1)
    with jax.named_scope("p_wkload"):
        loads[0].wait()

    def spread(c):
        along_y(a, c).start()
        each(1, depth, lambda t: along_z(t, c).start())

    spread(0)
    with jax.named_scope("p_hidload"):
        for load in loads[1:4]:
            load.wait()
    length = lengths[0]
    picks = lax.broadcasted_iota(jnp.int32, (16, seq_len), 1) == length - 1
    picks = jnp.where(picks, 1.0, 0.0).astype(BF16)
    row = jnp.concatenate(
        [
            jnp.dot(picks, hid[:, g * slab:(g + 1) * slab], preferred_element_type=F32)[:1]
            for g in range(n)
        ],
        axis=1,
    )
    scale = lax.rsqrt(jnp.mean(row * row, axis=-1, keepdims=True) + 1e-05)
    row_normed = (row * scale * again[...]).astype(BF16).astype(F32)
    size = jnp.full((1, 128), length, jnp.int32).astype(F32)
    for g in range(n):
        x_send[g, :, :slab] = row_normed[:, g * slab:(g + 1) * slab]
        x_send[g, :, slab:2 * slab] = row[:, g * slab:(g + 1) * slab]
        x_send[g, :, 2 * slab:] = size
    place = core * n + f
    with jax.named_scope("p_x"):
        each(1, n, lambda t: give(0, x_send.at[wrap(f + t, n)], x_recv.at[place], (dp, wrap(f + t, n))))
        for c in range(1, len(chunks)):
            spread(c)
        x_recv[place] = x_send[f]

    block = 32
    blocks = seq_len // block

    def square(i, carry):
        window = pl.ds(pl.multiple_of(i * block, block), block)
        x = hid[window, :].astype(F32)
        x = x * x
        lane_sum = x[:, :128]
        for k in range(1, width // 128):
            lane_sum += x[:, k * 128:(k + 1) * 128]
        squares[window, :] = lane_sum
        return carry

    with jax.named_scope("p_norm"):
        lax.fori_loop(0, blocks, square, 0)
        means = jnp.sum(squares[...], axis=-1, keepdims=True) / width
        squares[...] = jnp.broadcast_to(lax.rsqrt(means + 1e-05), squares.shape)

        def normalise(i, carry):
            window = pl.ds(pl.multiple_of(i * block, block), block)
            into = pl.ds(pl.multiple_of(core * seq_len + i * block, block), block)
            r = squares[window, :1]
            normed[into, :] = (hid[window, :].astype(F32) * r * again[...]).astype(BF16)
            return carry

        quarter = seq_len // 4

        def hand(k):
            part = normed.at[pl.ds(pl.multiple_of(core * seq_len + k * quarter, quarter), quarter), :]
            return pltpu.make_async_remote_copy(
                src_ref=part, dst_ref=part, send_sem=norm_send.at[k], recv_sem=norm_recv.at[k],
                device_id=(partner, f), device_id_type=MESH,
            )

        for k in range(4):
            lax.fori_loop(k * blocks // 4, (k + 1) * blocks // 4, normalise, 0)
            hand(k).start()

    def handed():
        for k in range(4):
            part = normed.at[pl.ds(pl.multiple_of((1 - core) * seq_len + k * quarter, quarter), quarter), :]
            pltpu.make_async_copy(part, part, norm_recv.at[k]).wait()

    def hand_rows():
        part = x_recv.at[pl.ds(pl.multiple_of(core * n, n), n)]
        return pltpu.make_async_remote_copy(
            src_ref=part, dst_ref=part, send_sem=norm_send.at[4], recv_sem=norm_recv.at[4],
            device_id=(partner, f), device_id_type=MESH,
        )

    def partial_queries():
        loads[4].wait()
        part = x_recv.at[pl.ds(pl.multiple_of((1 - core) * n, n), n)]
        pltpu.make_async_copy(part, part, norm_recv.at[4]).wait()
        x_all = jnp.concatenate([x_recv[k, :, :slab] for k in range(2 * n)], axis=0).astype(BF16)
        for h in range(MY_HEADS):
            part = jnp.dot(x_all, wq[:, h * HEAD:(h + 1) * HEAD], preferred_element_type=F32)
            for s in range(CORES):
                q_send[pl.ds(s * MY_HEADS + h, n, stride=CORES * MY_HEADS), :] = part[s * n:(s + 1) * n]
        rows = CORES * MY_HEADS

        def at(g):
            return pl.ds(pl.multiple_of(g * rows, rows), rows)

        each(1, n, lambda t: give(1, q_send.at[at(wrap(f + t, n))], q_recv.at[f], (dp, wrap(f + t, n))))
        q_recv[f] = q_send[at(f), :]

    def codes():
        for load in loads[5:]:
            load.wait()
        for i in range(n):
            last_in[i:i + 1, :] = x_recv[core * n + i][:, slab:2 * slab]
        lists = lax.broadcasted_iota(jnp.int32, (n, owners.shape[1]), 1)
        rows = lax.broadcasted_iota(jnp.int32, (n, owners.shape[1]), 0)
        ids = jnp.zeros((n, owners.shape[1]), jnp.int32)
        for r in range(n):
            ids = jnp.where(rows == r, list_ids[r], ids)
        owner = jnp.sum(jnp.where(lists == ids, owners[...], 0).astype(F32), axis=1, keepdims=True)
        lane = lax.broadcasted_iota(jnp.int32, (n, 128), 1)
        line = lax.broadcasted_iota(jnp.int32, (n, 128), 0)
        owner_row = jnp.sum(jnp.where(lane == line, owner, 0.0), axis=0, keepdims=True)
        earlier = jnp.where((owner_row == owner) & (lane < line), 1.0, 0.0)
        slot = jnp.sum(earlier, axis=1, keepdims=True)
        e_send[:, slab:] = jnp.broadcast_to(owner * cap + slot, (n, 128))

    split = 2 * unit
    parted = split % 128 == 0

    def accumulate(s, low, high):
        columns = pl.ds(pl.multiple_of(s * slab + low, 128), high - low)
        acc[...] += jnp.dot(normed[:, columns], wk[s, low:high, :], preferred_element_type=F32)

    assert len(shared) >= 2 or n > 8

    def own_plane(c):
        from_y(a, c).wait_recv()
        if c < n_alone:
            along_x(a, 1 - b, c).start()

    def pass_z(c):
        def body(pa):
            from_z(pa, c).wait_recv()
            along_y(pa, c).start()
            if c < n_alone:
                along_x(pa, b, c).start()
        others(body)

    def pass_y(c):
        def body(pa):
            from_y(pa, c).wait_recv()
            if c < n_alone:
                along_x(pa, 1 - b, c).start()
        others(body)

    last_chunk = len(chunks) - 1
    low, high = (0, split) if parted else (0, slab)

    def first_part(s, ready):
        for c in range(n_alone):
            ready(c)
        if parted:
            accumulate(s, split, slab)

    with jax.named_scope("g_0"):
        own_plane(0)
        pass_z(0)
    with jax.named_scope("g_rows"):
        arrived(0, x_recv, n - 1)
        hand_rows().start()
    acc[...] = jnp.zeros_like(acc)
    for c in range(1, len(chunks)):
        with jax.named_scope(f"g_z{c}"):
            own_plane(c)
            pass_z(c)
        with jax.named_scope(f"g_y{c}"):
            if c < last_chunk:
                pass_y(c - 1)
        if c == 1:
            with jax.named_scope("g_q"):
                partial_queries()
                codes()
        if c == min(2, last_chunk):
            with jax.named_scope("g_own"):
                handed()
                accumulate(f, 0, slab)
    with jax.named_scope("g_plane"):
        for c in range(n_alone):
            from_x(a, 1 - b, c).wait_recv()
        accumulate(a * 2 + 1 - b, 0, slab)
    with jax.named_scope("g_x"):
        others(lambda pa: first_part(pa * 2 + b, lambda c: from_x(pa, b, c).wait_recv()))
    with jax.named_scope("g_last"):
        pass_y(last_chunk - 1)
        pass_y(last_chunk)
    with jax.named_scope("g_xy"):
        others(lambda pa: first_part(pa * 2 + 1 - b, lambda c: from_x(pa, 1 - b, c).wait_recv()))
    with jax.named_scope("g_end"):
        if parted:
            for t in range(1, depth):
                shards = [far(t) * 2 + pb for pb in range(2)]
                left = jnp.concatenate([normed[:, pl.ds(pl.multiple_of(s * slab, 128), split)] for s in shards], axis=1)
                right = jnp.concatenate([wk[s, :split, :] for s in shards], axis=0)
                acc[...] += jnp.dot(left, right, preferred_element_type=F32)
        else:
            others(lambda pa: (accumulate(pa * 2 + b, low, high), accumulate(pa * 2 + 1 - b, low, high)) and None)

    with jax.named_scope("p_qwait"):
        arrived(1, q_recv, n - 1)
    queries = jnp.sum(q_recv[...], axis=0)
    rows = CORES * MY_HEADS
    upper = lax.broadcasted_iota(jnp.int32, (rows, 1), 0) >= MY_HEADS
    size_of = [x_recv[s * n + f][:, 2 * slab:2 * slab + 1] for s in range(CORES)]
    turns = []
    for s in range(CORES):
        token = lax.broadcasted_iota(jnp.int32, cos_t.shape, 0).astype(F32)
        at_last = token == size_of[s] - 1.0
        turns.append([
            jnp.sum(jnp.where(at_last, table[...], 0.0), axis=0, keepdims=True) for table in (cos_t, sin_t)
        ])
    q_cos = jnp.where(upper, turns[1][0], turns[0][0])
    q_sin = jnp.where(upper, turns[1][1], turns[0][1])
    queries = queries * q_cos + pltpu.roll(queries, HEAD // 2, 1) * q_sin
    queries = (queries * (1.0 / math.sqrt(HEAD))).astype(BF16)

    scores = jnp.zeros((rows, seq_len), F32)
    key_of = lax.broadcasted_iota(jnp.int32, scores.shape, 0) // GROUP
    for s in range(CORES):
        for kv in range(MY_KV):
            keys = acc[s * seq_len:(s + 1) * seq_len, kv * HEAD:(kv + 1) * HEAD]
            keys = (keys * cos_t[...] + pltpu.roll(keys, HEAD // 2, 1) * sin_t[...]).astype(BF16)
            part = lax.dot_general(queries, keys, (((1,), (1,)), ((), ())), preferred_element_type=F32)
            scores = jnp.where(key_of == s * MY_KV + kv, part, scores)
    token = lax.broadcasted_iota(jnp.int32, scores.shape, 1).astype(F32)
    visible = token < jnp.where(upper, size_of[1], size_of[0])
    scores = jnp.where(visible, scores, -jnp.inf)
    powers = jnp.exp(scores - jnp.max(scores, axis=-1, keepdims=True))
    weights = powers / jnp.sum(powers, axis=-1, keepdims=True)
    weights = jnp.concatenate(
        [jnp.where(upper, 0.0, weights), jnp.where(upper, weights, 0.0)], axis=1
    ).astype(BF16)

    spread_order = sorted(range(1, n), key=lambda t: (abs(t - half), t))

    def weighted(g):
        return jnp.dot(weights, normed[:, lanes(g, slab)], preferred_element_type=F32)

    with jax.named_scope("p_u"):
        for t in spread_order:
            g = wrap(f + t, n)
            u_send[g] = weighted(g).astype(BF16)
            give(2, u_send.at[g], u_recv.at[f], (dp, g))
        u_recv[f] = weighted(f).astype(BF16)
    with jax.named_scope("p_uwait"):
        arrived(2, u_recv, n - 1)
    sums = u_recv[...].reshape(n * rows, slab)
    product = jnp.dot(sums, wv[...], preferred_element_type=F32)
    for kv in range(MY_KV):
        mixed[kv] = product[:, kv * HEAD:(kv + 1) * HEAD]

    share = HEADS * HEAD // n
    for s in range(CORES):
        for h in range(MY_HEADS):
            part = mixed[h // GROUP, pl.ds(s * MY_HEADS + h, n, stride=rows), :]
            if share >= HEAD:
                at = h * HEAD % share
                c_send[s * half + h * HEAD // share, :, at:at + HEAD] = part
            else:
                pieces = HEAD // share
                for i in range(pieces):
                    c_send[s * half + h * pieces + i] = part[:, i * share:(i + 1) * share]

    mine = f // half == core
    other_core = 1 - core

    def context_to(s, t):
        k = lax.rem(f + t, half)
        give(3, c_send.at[s * half + k], c_recv.at[f], (base + s, core * half + k))

    each(1, half, lambda t: context_to(core, t))
    each(0, half, lambda t: context_to(other_core, t))

    @pl.when(mine)
    def _():
        c_recv[f] = c_send[core * half + lax.rem(f, half)]
        arrived(3, c_recv, n - 1)

    @pl.when(jnp.logical_not(mine))
    def _():
        context_to(core, 0)
        arrived(3, c_recv, n)

    context = jnp.sum(c_recv[...], axis=0).astype(BF16)

    def projected(g):
        return jnp.dot(context, wo[:, lanes(g, slab)], preferred_element_type=F32)

    with jax.named_scope("p_o"):
        for t in spread_order:
            g = wrap(f + t, n)
            o_send[g] = projected(g).astype(BF16)
            give(4, o_send.at[g], o_recv.at[f], (dp, g))
        o_recv[f] = projected(f).astype(BF16)
    with jax.named_scope("p_owait"):
        arrived(4, o_recv, n - 1)
    scaled = (last_in[...] + jnp.sum(o_recv[...].astype(F32), axis=0)) * fgain[...]
    lane = lax.broadcasted_iota(jnp.int32, (n, 128), 1)
    line = lax.broadcasted_iota(jnp.int32, (n, 128), 0)
    summed = jnp.sum(scaled * scaled, axis=1, keepdims=True)
    s_send[...] = jnp.sum(jnp.where(lane == line, summed, 0.0), axis=0, keepdims=True)
    everyone(lambda o, g: give(6, s_send, s_recv.at[me], (o, g)))
    e_send[:, :slab] = scaled
    for t in range(1, n_dp):
        give(5, e_send, e_recv.at[dp], (wrap(dp + t, n_dp), f))
    s_recv[me] = s_send[...]
    e_recv[dp] = e_send[...]
    with jax.named_scope("p_ewait"):
        arrived(5, e_recv, n_dp - 1)
        arrived(6, s_recv, total - 1)

    first = (dp * cap).astype(F32)
    for j in range(n_dp):
        sum_row = jnp.sum(s_recv[j * n:(j + 1) * n], axis=0)
        squared = jnp.sum(jnp.where(lane == line, sum_row, 0.0), axis=1, keepdims=True)
        embedded = e_recv[j, :, :slab] * lax.rsqrt(squared / width + 1e-06)
        embedded = embedded.astype(BF16).astype(F32)
        owner_slot = e_recv[j, :, slab:slab + 1]
        for s in range(cap):
            kept = jnp.where(owner_slot == first + s, embedded, 0.0)
            out_ref[0, j, s:s + 1, :] = jnp.sum(kept, axis=0, keepdims=True).astype(BF16)

    with jax.named_scope("p_sent"):
        hand_rows().wait_send()
        for slot, recv in ((0, x_recv), (1, q_recv), (2, u_recv), (4, o_recv)):
            sent(slot, recv, n - 1)

        @pl.when(mine)
        def _():
            sent(3, c_recv, n - 1)

        @pl.when(jnp.logical_not(mine))
        def _():
            sent(3, c_recv, n)

        sent(5, e_recv, n_dp - 1)
        sent(6, s_recv, total - 1)
        for k in range(4):
            hand(k).wait_send()
    with jax.named_scope("p_drain"):
        for c in range(len(chunks)):
            each(1, depth, lambda t: along_z(t, c).wait_send())
            each(0, depth, lambda t: along_y(far(t), c).wait_send())
            if c < n_alone:
                along_x(a, 1 - b, c).wait_send()
                others(lambda pa: (along_x(pa, b, c).wait_send(), along_x(pa, 1 - b, c).wait_send()) and None)


def local(
    n_dp, n,
    hidden, lengths, list_ids, list_owner, attn_gain, final_gain, w_query, w_key, w_value, w_out,
):
    _, seq_len, width = hidden.shape
    slab = width // n
    depth = n // 2
    cap = max(2, 2 * n // n_dp)
    share = HEADS * HEAD // n
    cosine, sine = rope_tables(seq_len)
    alone, shared = key_chunks(n)
    dma = pltpu.SemaphoreType.DMA
    any_spec = pl.BlockSpec(memory_space=pl.ANY)
    vmem = pltpu.VMEM
    key_width = w_key.shape[1] // CORES
    rows = CORES * MY_HEADS
    return pl.pallas_call(
        functools.partial(kernel, n_dp, n),
        out_shape=jax.ShapeDtypeStruct((1, n_dp, cap, slab), BF16),
        in_specs=[any_spec] * 12,
        out_specs=pl.BlockSpec(memory_space=pltpu.VMEM),
        scratch_shapes=[
            pltpu.SMEM(lengths.shape, jnp.int32),
            pltpu.SMEM(list_ids.shape, jnp.int32),
            vmem((seq_len, width), BF16),
            vmem((CORES * seq_len, width), BF16),
            vmem((seq_len, 128), F32),
            vmem((1, width), F32),
            vmem((1, slab), F32),
            vmem((seq_len, HEAD), F32),
            vmem((seq_len, HEAD), F32),
            vmem((w_query.shape[0], w_query.shape[1] // CORES), BF16),
            vmem((n, slab, key_width), BF16),
            vmem((slab, key_width), BF16),
            vmem(w_out.shape, BF16),
            vmem((1, list_owner.shape[0]), jnp.int32),
            vmem((CORES * seq_len, key_width), F32),
            vmem((n, slab), F32),
            vmem((n, 1, 2 * slab + 128), F32),
            vmem((CORES * n, 1, 2 * slab + 128), F32),
            vmem((n * rows, HEAD), F32),
            vmem((n, rows, HEAD), F32),
            vmem((n, rows, slab), BF16),
            vmem((n, rows, slab), BF16),
            vmem((MY_KV, n * rows, HEAD), F32),
            vmem((n, n, share), F32),
            vmem((n, n, share), F32),
            vmem((n, n, slab), BF16),
            vmem((n, n, slab), BF16),
            vmem((n, slab + 128), F32),
            vmem((n_dp, n, slab + 128), F32),
            vmem((1, 128), F32),
            vmem((n_dp * n, 1, 128), F32),
            dma((12,)),
            dma((7,)),
            dma((7,)),
            dma((5,)),
            dma((5,)),
            dma((depth, len(alone) + len(shared))),
            dma((depth, len(alone) + len(shared))),
            dma((n, len(alone))),
            dma((depth, len(alone) + len(shared))),
            dma((depth, len(alone) + len(shared))),
            dma((n, len(alone))),
        ],
        compiler_params=pltpu.CompilerParams(
            collective_id=0, has_side_effects=True, vmem_limit_bytes=67043328
        ),
    )(
        lengths, list_ids,
        list_owner.reshape(1, -1), hidden, attn_gain.reshape(1, width), final_gain.reshape(1, width),
        cosine, sine, w_query, w_key, w_value, w_out,
    )


def solution(mesh):
    in_specs = (
        P(("dp", "fsdp"), None, None),
        P(("dp", "fsdp")),
        P("dp"),
        P(),
        P(),
        P(),
        P("fsdp", None),
        P("fsdp", None),
        P("fsdp", None),
        P("fsdp", None),
    )
    out_specs = P("dp", None, None, "fsdp")
    body = functools.partial(local, mesh.shape["dp"], mesh.shape["fsdp"])
    return jax.shard_map(body, mesh=mesh, in_specs=in_specs, out_specs=out_specs, check_vma=False)
```
